32 devices in a mesh: pod: 1 (over z), data: 4 (over y), col: 4 (over x), row: 2 (over core).
Axes of the slice: x: 4, y: 4, z: 1, core: 2. Of those that a mesh axis runs over, the one named last changes fastest.
The devices are a block of a 4x4x8 slice.
Arguments:
- x_act: bfloat16 [8192, 2048], P(('pod', 'data', 'row'), 'col')
- w_fused: bfloat16 [2048, 22016], P(('pod', 'row'), 'col')
- dy_out: bfloat16 [8192, 22016], P(('pod', 'data', 'row'), 'col')
Outputs:
- output 1: bfloat16 [8192, 2048], P(('pod', 'data', 'row'), 'col')
- output 2: float32 [2048, 22016], P(('pod', 'data', 'row'), 'col')
All inputs are finite; a program needn't handle non-finite values.
Results may differ from the reference program's by a relative error of at most 0.001.
Values are sent between devices in bfloat16 or wider.
A program may use at most 768 MiB of HBM per device.

```python
import jax
import jax.numpy as jnp

HIDDEN = 2048
OUT_COLS = 22016
ROW_COUNT = 8192


def setup_inputs(seed: int = 0, part: int = 0) -> dict:
    part_key = jax.random.fold_in(jax.random.key(seed), part)
    key_act, key_wgt, key_grad = jax.random.split(part_key, 3)
    act_vals = jax.random.normal(key_act, (ROW_COUNT, HIDDEN), jnp.float32) * ROW_COUNT ** -0.5
    wgt_vals = jax.random.normal(key_wgt, (HIDDEN, OUT_COLS), jnp.float32) * OUT_COLS ** -0.5
    grad_vals = jax.random.normal(key_grad, (ROW_COUNT, OUT_COLS), jnp.float32)
    return {"x_act": act_vals.astype(jnp.bfloat16), "w_fused": wgt_vals.astype(jnp.bfloat16), "dy_out": grad_vals.astype(jnp.bfloat16)}


def reference(x_act, w_fused, dy_out):
    dx_full = jnp.dot(dy_out, w_fused.T, preferred_element_type=jnp.float32)
    dw_full = jnp.dot(x_act.T, dy_out, preferred_element_type=jnp.float32)
    return dx_full.astype(jnp.bfloat16), dw_full
```

```python
import functools

import jax
import jax.numpy as jnp
from jax import lax
from jax.experimental import pallas as pl
from jax.experimental.pallas import tpu as pltpu
from jax.sharding import PartitionSpec as P

MESH = pl.DeviceIdType.MESH
F32, BF16 = jnp.float32, jnp.bfloat16

ARRIVAL = ((0, 0), (0, 1), (1, 0), (3, 1), (1, 1), (3, 0), (2, 0), (2, 1))
WIDE = 1024
TILE = 256
DEPTH = 512


def kernel(nd, nc, x_ref, w_ref, dy_ref, dx_ref, dw_ref, dyo, wo, tail_y,
           xg, xt, part, relay_y, acc, relay_x, tail_x, buf, stage,
           sem_g, rem_g, sem_gp, sem_gf, loc_x, sem_a, rem_a, sem_w, rem_w, loc_d,
           sem_y, rem_y, sem_x, rem_x, loc_s, loc_o, loc_w, loc_dx):
    d, c, r = lax.axis_index("data"), lax.axis_index("col"), lax.axis_index("row")
    tokens, cols = dy_ref.shape
    half = xg.shape[3]
    band = 2 * half
    d_up, d_dn = (d + 1) % nd, (d + nd - 1) % nd
    c_up, c_dn = (c + 1) % nc, (c + nc - 1) % nc
    other = 1 - r
    mine = pl.ds(pl.multiple_of(r * tokens, tokens), tokens)
    theirs = pl.ds(pl.multiple_of(other * tokens, tokens), tokens)
    chunks = [(lo, min(WIDE, cols - lo)) for lo in range(0, cols, WIDE)]

    def rcopy(src, dst, send, recv, **to):
        return pltpu.make_async_remote_copy(src_ref=src, dst_ref=dst, send_sem=send, recv_sem=recv,
                                            device_id=to, device_id_type=MESH)

    def lcopy(src, dst, sem):
        return pltpu.make_async_copy(src, dst, sem)

    def x_local(t):
        return lcopy(x_ref.at[:, pl.ds(pl.multiple_of(r * band + t * half, half), half)], xg.at[0, t, mine], loc_x.at[t])

    def x_partner(t):
        return rcopy(x_ref.at[:, pl.ds(pl.multiple_of(other * band + t * half, half), half)], xg.at[0, t, mine],
                     sem_gp.at[t], rem_g.at[0, t, r], row=other)

    def x_send(up, core, t):
        slot = 3 if up else 1
        return rcopy(x_ref.at[:, pl.ds(core * band + t * half, half)], xg.at[slot, t, mine],
                     sem_g.at[up, core, t], rem_g.at[slot, t, r], col=c_up if up else c_dn, row=core)

    def x_pass(up, t):
        src, rows, who = (3, pl.ds(0, tokens), 0) if up else (1, pl.ds(tokens, tokens), 1)
        return rcopy(xg.at[src, t, rows], xg.at[2, t, rows], sem_gf.at[up, t], rem_g.at[2, t, who],
                     col=c_up if up else c_dn)

    def x_arrived(k, t, who):
        rows = pl.ds(pl.multiple_of(who * tokens, tokens), tokens)
        return rcopy(xg.at[k, t, rows], xg.at[k, t, rows], sem_gp.at[0], rem_g.at[k, t, who], row=other)

    def dy_swap(j):
        lo, w = chunks[j]
        dst = buf.at[j, mine, pl.ds(0, w)] if j < 2 else dyo.at[:, pl.ds(lo, w)]
        return rcopy(dy_ref.at[:, pl.ds(lo, w)], dst, sem_a.at[j], rem_a.at[j], row=other)

    def dy_arrived(j):
        lo, w = chunks[j]
        dst = buf.at[j, theirs, pl.ds(0, w)] if j < 2 else dyo.at[:, pl.ds(lo, w)]
        return rcopy(dy_ref.at[:, pl.ds(lo, w)], dst, sem_a.at[j], rem_a.at[j], row=other)

    def dy_load(j):
        lo, w = chunks[j]
        return lcopy(dy_ref.at[:, pl.ds(lo, w)], buf.at[j % 2, mine, pl.ds(0, w)], loc_d.at[j % 2, 0])

    def dyo_load(j):
        lo, w = chunks[j]
        return lcopy(dyo.at[:, pl.ds(lo, w)], buf.at[j % 2, theirs, pl.ds(0, w)], loc_d.at[j % 2, 1])

    def w_swap():
        return rcopy(w_ref, wo, sem_w, rem_w, row=other)

    def y_msg(m, j):
        at = pl.ds(*chunks[j])
        k, t = ((2, 1), (2, 0), (1, 0), (3, 1), (1, 1), (3, 0))[m]
        down = m % 2
        dst = relay_y.at[down, :, at] if m < 2 else tail_y.at[t, down, :, at]
        return rcopy(part.at[k, t, :, at], dst, sem_y.at[m, j], rem_y.at[m, j], data=d_dn if down else d_up)

    def x_msg(m):
        k, t = ((2, 1), (2, 0), (1, 0), (3, 1), (1, 1), (3, 0))[m]
        down = m % 2
        dst = relay_x.at[down] if m < 2 else tail_x.at[t, down]
        return rcopy(acc.at[k, t], dst, sem_x.at[m], rem_x.at[m], col=c_dn if down else c_up)

    for t in range(2):
        x_local(t).start()
    for j in range(2):
        dy_load(j).start()

    barrier = pltpu.get_barrier_semaphore()
    peers = [dict(row=other), dict(data=d_up), dict(data=d_dn)]
    peers += [dict(col=n, row=k) for n in (c_up, c_dn) for k in range(2)]
    for peer in peers:
        pl.semaphore_signal(barrier, inc=1, device_id=peer, device_id_type=MESH)
    pl.semaphore_wait(barrier, len(peers))

    for t in range(2):
        x_partner(t).start()
    dy_swap(0).start()
    for turn in range(2):
        for core in range(2):
            x_send(1, core, 1 - turn).start()
            x_send(0, core, turn).start()
    for j in range(1, len(chunks)):
        dy_swap(j).start()
    w_swap().start()

    def turn_block(i):
        k, t = ARRIVAL[i]

        def step(b, _):
            rows = pl.ds(pl.multiple_of(b * 512, 512), 512)
            xt[i, :, rows] = xg[k, t, rows, :].T
            return 0

        lax.fori_loop(0, 2 * tokens // 512, step, 0)

    def product(first, count, j):
        lo, w = chunks[j]

        def one(at, width):
            lhs = xt[first:first + count].reshape(count * half, 2 * tokens)
            rhs = buf[j % 2, :, pl.ds(at, width)]
            out = lax.dot_general(lhs, rhs, (((1,), (0,)), ((), ())), preferred_element_type=F32)
            for n in range(count):
                k, t = ARRIVAL[first + n]
                part[(k + c - d + nd) % nd, t, :, pl.ds(pl.multiple_of(lo + at, 128), width)] = out[n * half:(n + 1) * half]

        def step(b, _):
            one(pl.multiple_of(b * TILE, TILE), TILE)
            return 0

        lax.fori_loop(0, w // TILE, step, 0)
        if w % TILE:
            one(w - w % TILE, w % TILE)

    early = min(2, len(chunks))
    for s in range(4):
        for i in (2 * s, 2 * s + 1):
            k, t = ARRIVAL[i]
            if k == 0:
                x_local(t).wait()
                x_arrived(0, t, other).wait_recv()
            else:
                for who in range(2):
                    x_arrived(k, t, who).wait_recv()
            if k == 3:
                x_pass(1, t).start()
            if k == 1:
                x_pass(0, t).start()
        for i in (2 * s, 2 * s + 1):
            turn_block(i)
        for j in range(early):
            if s == 0:
                dy_load(j).wait()
                dy_arrived(j).wait_recv()
            product(2 * s, 2, j)
            for i in (2 * s, 2 * s + 1):
                k, t = ARRIVAL[i]
                near = (k + c - d + nd) % nd
                for when, m in ((2, 0 if t else 1), (3 if t else 1, 3 if t else 2)):
                    @pl.when(near == when)
                    def _(m=m, j=j):
                        y_msg(m, j).start()

    def refill(j):
        if j < len(chunks):
            dy_arrived(j).wait_recv()
            dy_load(j).start()
            dyo_load(j).start()

    refill(2)
    refill(3)
    for j in range(early, len(chunks)):
        dy_load(j).wait()
        dyo_load(j).wait()
        product(0, 4, j)
        product(4, 4, j)
        for m in range(4):
            y_msg(m, j).start()
        refill(j + 2)

    w_swap().wait_recv()
    steps = cols // DEPTH
    rest = cols - steps * DEPTH

    def dx_loads(slot, lo, w):
        at, to = pl.ds(lo, w), pl.ds(pl.multiple_of(slot * DEPTH, DEPTH), w)
        return (lcopy(w_ref.at[:, at], buf.at[0, mine, to], loc_w.at[slot, 0]),
                lcopy(wo.at[:, at], buf.at[0, theirs, to], loc_w.at[slot, 1]),
                lcopy(dy_ref.at[:, at], buf.at[1, pl.ds(0, tokens), to], loc_w.at[slot, 2]))

    quarter = acc.shape[3]
    deep = acc.shape[2]

    def dx_product(slot, w, fresh):
        to = pl.ds(pl.multiple_of(slot * DEPTH, DEPTH), w)

        def step(b, _):
            k, h = b // 2, b % 2
            rows = pl.multiple_of((c + k) % nc * quarter + h * TILE, TILE)
            cut = pl.ds(pl.multiple_of(h * TILE, TILE), TILE)
            for t in range(2):
                out = lax.dot_general(buf[1, t * deep:(t + 1) * deep, to], buf[0, pl.ds(rows, TILE), to],
                                      (((1,), (1,)), ((), ())), preferred_element_type=F32)
                if fresh:
                    acc[k, t, :, cut] = out
                else:
                    acc[k, t, :, cut] += out
            return 0

        lax.fori_loop(0, nc * quarter // TILE, step, 0)

    def dx_at(i):
        return pl.multiple_of(i * DEPTH, 128)

    for copy in dx_loads(0, steps * DEPTH, rest) + dx_loads(1, dx_at(0), DEPTH):
        copy.start()
    for copy in dx_loads(0, steps * DEPTH, rest):
        copy.wait()
    dx_product(0, rest, True)

    def dx_step(i, _):
        slot = (i + 1) % 2

        @pl.when(i + 1 < steps)
        def _():
            for copy in dx_loads(i % 2, dx_at(i + 1), DEPTH):
                copy.start()

        for copy in dx_loads(slot, dx_at(i), DEPTH):
            copy.wait()
        dx_product(slot, DEPTH, False)
        return 0

    lax.fori_loop(0, steps, dx_step, 0)
    for m in range(4):
        x_msg(m).start()

    def pass_y(j):
        at = pl.ds(*chunks[j])
        for down, k, t in ((0, 1, 1), (1, 3, 0)):
            y_msg(down, j).wait_recv()
            part[k, t, :, at] += relay_y[down, :, at]
            y_msg(4 + down, j).start()

    def pass_x():
        for down, k, t in ((0, 1, 1), (1, 3, 0)):
            x_msg(down).wait_recv()
            acc[k, t] += relay_x[down]
            x_msg(4 + down).start()

    for j in range(len(chunks) - 1):
        pass_y(j)
    pass_x()
    pass_y(len(chunks) - 1)

    def done_x():
        for t in range(2):
            for m in ((2, 5) if t == 0 else (3, 4)):
                x_msg(m).wait_recv()
            rows = pl.ds(t * deep, deep)
            buf[1, rows, 0:quarter] = (acc[0, t] + tail_x[t, 0] + tail_x[t, 1]).astype(BF16)
            lcopy(buf.at[1, rows, pl.ds(0, quarter)], dx_ref.at[rows], loc_dx.at[t]).start()

    def done_y(j):
        lo, w = chunks[j]
        at = pl.ds(lo, w)
        for m in range(2, 6):
            y_msg(m, j).wait_recv()
        loads = [lcopy(tail_y.at[t, down, :, at], stage.at[t, down, :, pl.ds(0, w)], loc_s.at[t, down])
                 for t in range(2) for down in range(2)]
        for copy in loads:
            copy.start()
        for copy in loads:
            copy.wait()
        for t in range(2):
            part[0, t, :, at] += stage[t, 0, :, 0:w] + stage[t, 1, :, 0:w]
            out_y(t, j).start()

    def out_y(t, j):
        at = pl.ds(*chunks[j])
        return lcopy(part.at[0, t, :, at], dw_ref.at[pl.ds(t * half, half), at], loc_o.at[t, j])

    done_y(0)
    done_x()
    for j in range(1, len(chunks)):
        done_y(j)

    for t in range(2):
        x_partner(t).wait_send()
        for up in range(2):
            x_pass(up, t).wait_send()
            for core in range(2):
                x_send(up, core, t).wait_send()
        rows = pl.ds(t * deep, deep)
        lcopy(buf.at[1, rows, pl.ds(0, quarter)], dx_ref.at[rows], loc_dx.at[t]).wait()
    w_swap().wait_send()
    for m in range(6):
        x_msg(m).wait_send()
    for j in range(len(chunks)):
        dy_swap(j).wait_send()
        for m in range(6):
            y_msg(m, j).wait_send()
        for t in range(2):
            out_y(t, j).wait()


def solution(mesh):
    act_spec = P(("pod", "data", "row"), "col")
    wgt_spec = P(("pod", "row"), "col")
    nd, nc = mesh.shape["data"], mesh.shape["col"]

    def local_step(x_blk, w_blk, dy_blk):
        tokens, feats = x_blk.shape
        cols = dy_blk.shape[1]
        deep = w_blk.shape[0] * 2 // nd // 2
        half = deep // 2
        count = pl.cdiv(cols, WIDE)
        any_spec = pl.BlockSpec(memory_space=pl.ANY)
        dma = pltpu.SemaphoreType.DMA
        outs = pl.pallas_call(
            functools.partial(kernel, nd, nc),
            out_shape=(
                jax.ShapeDtypeStruct((tokens, feats), BF16),
                jax.ShapeDtypeStruct((deep, cols), F32),
                jax.ShapeDtypeStruct((tokens, cols), BF16),
                jax.ShapeDtypeStruct(w_blk.shape, BF16),
                jax.ShapeDtypeStruct((2, 2, half, cols), F32),
            ),
            in_specs=[any_spec] * 3,
            out_specs=(any_spec,) * 5,
            scratch_shapes=[
                pltpu.VMEM((4, 2, 2 * tokens, half), BF16),
                pltpu.VMEM((8, half, 2 * tokens), BF16),
                pltpu.VMEM((4, 2, half, cols), F32),
                pltpu.VMEM((2, half, cols), F32),
                pltpu.VMEM((4, 2, tokens // 2, feats), F32),
                pltpu.VMEM((2, tokens // 2, feats), F32),
                pltpu.VMEM((2, 2, tokens // 2, feats), F32),
                pltpu.VMEM((2, 2 * tokens, WIDE), BF16),
                pltpu.VMEM((2, 2, half, WIDE), F32),
                dma((2, 2, 2)), dma((4, 2, 2)), dma((2,)), dma((2, 2)), dma((2,)),
                dma((count,)), dma((count,)), dma(()), dma(()), dma((2, 2)),
                dma((6, count)), dma((6, count)), dma((6,)), dma((6,)),
                dma((2, 2)), dma((2, count)), dma((2, 3)), dma((2,)),
            ],
            compiler_params=pltpu.CompilerParams(
                collective_id=0, has_side_effects=True, vmem_limit_bytes=67043328),
        )(x_blk, w_blk, dy_blk)
        return outs[0], outs[1]

    return jax.shard_map(local_step, mesh=mesh, in_specs=(act_spec, wgt_spec, act_spec),
                         out_specs=(act_spec, act_spec), check_vma=False)
```

```python
import functools

import jax
import jax.numpy as jnp
from jax import lax
from jax.experimental import pallas as pl
from jax.experimental.pallas import tpu as pltpu
from jax.sharding import PartitionSpec as P

MESH = pl.DeviceIdType.MESH
F32, BF16 = jnp.float32, jnp.bfloat16

ARRIVAL = ((0, 0), (0, 1), (1, 0), (3, 1), (1, 1), (3, 0), (2, 0), (2, 1))
WIDE = 1024
TILE = 256
DEPTH = 512


def split(cols):
    widths = [WIDE // 2] + [WIDE] * ((cols - WIDE // 2) // WIDE)
    rest = cols - sum(widths)
    widths += [WIDE // 2] * (rest > WIDE // 2) + [rest - WIDE // 2 * (rest > WIDE // 2)]
    return [(sum(widths[:i]), w) for i, w in enumerate(widths)]


def kernel(nd, nc, x_ref, w_ref, dy_ref, dx_ref, dw_ref, dyo, wo, tail_y,
           xl, xs, xt, part, relay_y, acc, relay_x, tail_x, buf, stage,
           sem_g, rem_g, sem_gp, sem_gf, loc_x, sem_a, rem_a, sem_v, rem_v, sem_w, rem_w, loc_d,
           sem_y, rem_y, sem_x, rem_x, loc_s, loc_o, loc_w, loc_dx):
    d, c, r = lax.axis_index("data"), lax.axis_index("col"), lax.axis_index("row")
    tokens, cols = dy_ref.shape
    half = xt.shape[1]
    piece = half // 2
    band = 2 * half
    d_up, d_dn = (d + 1) % nd, (d + nd - 1) % nd
    c_up, c_dn = (c + 1) % nc, (c + nc - 1) % nc
    other = 1 - r
    mine = pl.ds(pl.multiple_of(r * tokens, tokens), tokens)
    theirs = pl.ds(pl.multiple_of(other * tokens, tokens), tokens)
    chunks = split(cols)
    n = len(chunks)

    def rcopy(src, dst, send, recv, **to):
        return pltpu.make_async_remote_copy(src_ref=src, dst_ref=dst, send_sem=send, recv_sem=recv,
                                            device_id=to, device_id_type=MESH)

    def lcopy(src, dst, sem):
        return pltpu.make_async_copy(src, dst, sem)

    place = {block: i for i, block in enumerate(ARRIVAL)}

    def x_partner(t):
        return rcopy(xs.at[pl.ds(pl.multiple_of(other * band + t * half, half), half)], xt.at[place[0, t], :, mine],
                     sem_gp.at[t], rem_g.at[place[0, t], 0, r], row=other)

    def x_send(up, core, t, p):
        i = place[3 if up else 1, t]
        return rcopy(xs.at[pl.ds(core * band + t * half + p * piece, piece)], xt.at[i, pl.ds(p * piece, piece), mine],
                     sem_g.at[up, core, t, p], rem_g.at[i, p, r], col=c_up if up else c_dn, row=core)

    def x_pass(up, t):
        k, rows, who = (3, pl.ds(0, tokens), 0) if up else (1, pl.ds(tokens, tokens), 1)
        return rcopy(xt.at[place[k, t], :, rows], xt.at[place[2, t], :, rows], sem_gf.at[up, t],
                     rem_g.at[place[2, t], 0, who], col=c_up if up else c_dn)

    def x_arrived(i, p, who):
        k = ARRIVAL[i][0]
        cut = pl.ds(p * piece, piece) if k in (1, 3) else pl.ds(0, half)
        at = xt.at[i, cut, pl.ds(pl.multiple_of(who * tokens, tokens), tokens)]
        return rcopy(at, at, sem_gp.at[0], rem_g.at[i, p, who], row=other)

    def dy_swap(j):
        at = pl.ds(*chunks[j])
        return rcopy(dy_ref.at[:, at], dyo.at[:, at], sem_a.at[j], rem_a.at[j], row=other)

    def dy_direct(j, to):
        lo, w = chunks[j]
        return rcopy(dy_ref.at[:, pl.ds(lo, w)], buf.at[j, to, pl.ds(0, w)], sem_v.at[j], rem_v.at[j], row=other)

    def dy_load(j):
        lo, w = chunks[j]
        return lcopy(dy_ref.at[:, pl.ds(lo, w)], buf.at[j % 2, mine, pl.ds(0, w)], loc_d.at[j % 2, 0])

    def dyo_load(j):
        lo, w = chunks[j]
        return lcopy(dyo.at[:, pl.ds(lo, w)], buf.at[j % 2, theirs, pl.ds(0, w)], loc_d.at[j % 2, 1])

    def w_swap():
        return rcopy(w_ref, wo, sem_w, rem_w, row=other)

    def y_msg(m, j, p):
        at = pl.ds(*chunks[j])
        k, t = ((2, 1), (2, 0), (1, 0), (3, 1), (1, 1), (3, 0))[m]
        rows = pl.ds(p * piece, piece)
        down = m % 2
        dst = relay_y.at[down, rows, at] if m < 2 else tail_y.at[t, down, rows, at]
        return rcopy(part.at[k, t, rows, at], dst, sem_y.at[m, j, p], rem_y.at[m, j, p], data=d_dn if down else d_up)

    def x_msg(m):
        k, t = ((2, 1), (2, 0), (1, 0), (3, 1), (1, 1), (3, 0))[m]
        down = m % 2
        dst = relay_x.at[down] if m < 2 else tail_x.at[t, down]
        return rcopy(acc.at[k, t], dst, sem_x.at[m], rem_x.at[m], col=c_dn if down else c_up)

    x_load = lcopy(x_ref, xl, loc_x)
    x_load.start()
    for j in range(2):
        dy_load(j).start()

    barrier = pltpu.get_barrier_semaphore()
    peers = [dict(row=other), dict(data=d_up), dict(data=d_dn)]
    peers += [dict(col=n, row=k) for n in (c_up, c_dn) for k in range(2)]
    for peer in peers:
        pl.semaphore_signal(barrier, inc=1, device_id=peer, device_id_type=MESH)
    x_load.wait()
    for b in range(xl.shape[1] // 128):
        xs[b * 128:(b + 1) * 128, :] = xl[:, b * 128:(b + 1) * 128].T
    for t in range(2):
        xt[place[0, t], :, mine] = xs[pl.ds(pl.multiple_of(r * band + t * half, half), half), :]
    pl.semaphore_wait(barrier, len(peers))

    for p in range(2):
        for core in range(2):
            x_send(1, core, 1, p).start()
            x_send(0, core, 0, p).start()
        if p == 0:
            for t in range(2):
                x_partner(t).start()
            dy_direct(0, mine).start()
    for p in range(2):
        for core in range(2):
            x_send(1, core, 0, p).start()
            x_send(0, core, 1, p).start()
    dy_direct(1, mine).start()
    for j in (*range(2, n), 0, 1):
        dy_swap(j).start()
    w_swap().start()

    def product(first, count, j, lead=0, rows=half):
        lo, w = chunks[j]

        def one(at, width):
            lhs = xt[first:first + count, lead:lead + rows].reshape(count * rows, 2 * tokens)
            rhs = buf[j % 2, :, pl.ds(at, width)]
            out = lax.dot_general(lhs, rhs, (((1,), (0,)), ((), ())), preferred_element_type=F32)
            for i in range(count):
                k, t = ARRIVAL[first + i]
                part[(k + c - d + nd) % nd, t, lead:lead + rows, pl.ds(pl.multiple_of(lo + at, 128), width)] = out[i * rows:(i + 1) * rows]

        def step(b, _):
            one(pl.multiple_of(b * TILE, TILE), TILE)
            return 0

        lax.fori_loop(0, w // TILE, step, 0)
        if w % TILE:
            one(w - w % TILE, w % TILE)

    def send(first, count, j, pieces):
        for k, t in ARRIVAL[first:first + count]:
            near = (k + c - d + nd) % nd
            for when, m in ((2, 0 if t else 1), (3 if t else 1, 3 if t else 2)):
                @pl.when(near == when)
                def _(m=m):
                    for p in pieces:
                        y_msg(m, j, p).start()

    swapped = set()

    def refill(j):
        if j not in swapped:
            dy_swap(j).wait_recv()
            swapped.add(j)
        dy_load(j).start()
        dyo_load(j).start()

    def filled(j):
        dy_load(j).wait()
        dyo_load(j).wait()

    for t in range(2):
        x_arrived(place[0, t], 0, other).wait_recv()
    for j in range(2):
        dy_load(j).wait()
        dy_direct(j, theirs).wait_recv()
        product(0, 2, j)
        send(0, 2, j, (0, 1))
        if j == 0:
            for i in (2, 3):
                for who in range(2):
                    x_arrived(i, 0, who).wait_recv()
        product(2, 2, j, 0, piece)
        send(2, 2, j, (0,))
    for i in (2, 3):
        for who in range(2):
            x_arrived(i, 1, who).wait_recv()
    x_pass(1, 1).start()
    x_pass(0, 0).start()
    for j in range(2):
        product(2, 2, j, piece, piece)
        send(2, 2, j, (1,))
        refill(j + 2)
    for j in range(2, n):
        filled(j)
        product(0, 4, j)
        send(0, 4, j, (0, 1))
        if j + 2 < n:
            refill(j + 2)
    for i in (4, 5):
        for p in range(2):
            for who in range(2):
                x_arrived(i, p, who).wait_recv()
    x_pass(1, 0).start()
    x_pass(0, 1).start()
    refill(0)
    refill(1)
    for i in (6, 7):
        for who in range(2):
            x_arrived(i, 0, who).wait_recv()

    for j in range(n):
        filled(j)
        product(4, 4, j)
        send(4, 4, j, (0, 1))
        if j + 2 < n:
            refill(j + 2)

    w_swap().wait_recv()
    steps = cols // DEPTH
    rest = cols - steps * DEPTH

    def dx_loads(slot, lo, w):
        at, to = pl.ds(lo, w), pl.ds(pl.multiple_of(slot * DEPTH, DEPTH), w)
        return (lcopy(w_ref.at[:, at], buf.at[0, mine, to], loc_w.at[slot, 0]),
                lcopy(wo.at[:, at], buf.at[0, theirs, to], loc_w.at[slot, 1]),
                lcopy(dy_ref.at[:, at], buf.at[1, pl.ds(0, tokens), to], loc_w.at[slot, 2]))

    quarter = acc.shape[3]
    deep = acc.shape[2]

    def dx_product(slot, w, fresh):
        to = pl.ds(pl.multiple_of(slot * DEPTH, DEPTH), w)

        def step(b, _):
            k, h = b // 2, b % 2
            rows = pl.multiple_of((c + k) % nc * quarter + h * TILE, TILE)
            cut = pl.ds(pl.multiple_of(h * TILE, TILE), TILE)
            for t in range(2):
                out = lax.dot_general(buf[1, t * deep:(t + 1) * deep, to], buf[0, pl.ds(rows, TILE), to],
                                      (((1,), (1,)), ((), ())), preferred_element_type=F32)
                if fresh:
                    acc[k, t, :, cut] = out
                else:
                    acc[k, t, :, cut] += out
            return 0

        lax.fori_loop(0, nc * quarter // TILE, step, 0)

    def dx_at(i):
        return pl.multiple_of(i * DEPTH, 128)

    for copy in dx_loads(0, steps * DEPTH, rest) + dx_loads(1, dx_at(0), DEPTH):
        copy.start()
    for copy in dx_loads(0, steps * DEPTH, rest):
        copy.wait()
    dx_product(0, rest, True)

    def dx_step(i, _):
        slot = (i + 1) % 2

        @pl.when(i + 1 < steps)
        def _():
            for copy in dx_loads(i % 2, dx_at(i + 1), DEPTH):
                copy.start()

        for copy in dx_loads(slot, dx_at(i), DEPTH):
            copy.wait()
        dx_product(slot, DEPTH, False)
        return 0

    lax.fori_loop(0, steps, dx_step, 0)
    for m in range(4):
        x_msg(m).start()

    def pass_y(j):
        at = pl.ds(*chunks[j])
        for down, k, t in ((0, 1, 1), (1, 3, 0)):
            for p in range(2):
                rows = slice(p * piece, (p + 1) * piece)
                y_msg(down, j, p).wait_recv()
                part[k, t, rows, at] += relay_y[down, rows, at]
                y_msg(4 + down, j, p).start()

    def pass_x():
        for down, k, t in ((0, 1, 1), (1, 3, 0)):
            x_msg(down).wait_recv()
            acc[k, t] += relay_x[down]
            x_msg(4 + down).start()

    for j in range(n):
        pass_y(j)
    pass_x()

    def done_x():
        for t in range(2):
            for m in ((2, 5) if t == 0 else (3, 4)):
                x_msg(m).wait_recv()
            rows = pl.ds(t * deep, deep)
            buf[1, rows, 0:quarter] = (acc[0, t] + tail_x[t, 0] + tail_x[t, 1]).astype(BF16)
            lcopy(buf.at[1, rows, pl.ds(0, quarter)], dx_ref.at[rows], loc_dx.at[t]).start()

    def done_y(j):
        lo, w = chunks[j]
        at = pl.ds(lo, w)
        for m in range(2, 6):
            for p in range(2):
                y_msg(m, j, p).wait_recv()
        if j == len(chunks) - 1:
            return
        loads = [lcopy(tail_y.at[t, down, :, at], stage.at[t, down, :, pl.ds(0, w)], loc_s.at[t, down])
                 for t in range(2) for down in range(2)]
        for copy in loads:
            copy.start()
        for copy in loads:
            copy.wait()
        for t in range(2):
            part[0, t, :, at] += stage[t, 0, :, 0:w] + stage[t, 1, :, 0:w]
            out_y(t, j).start()

    def out_y(t, j):
        at = pl.ds(*chunks[j])
        return lcopy(part.at[0, t, :, at], dw_ref.at[pl.ds(t * half, half), at], loc_o.at[t, j])

    for t in range(2):
        out_y(t, len(chunks) - 1).start()
    done_x()
    for j in range(n):
        done_y(j)

    for t in range(2):
        x_partner(t).wait_send()
        for up in range(2):
            x_pass(up, t).wait_send()
            for core in range(2):
                for p in range(2):
                    x_send(up, core, t, p).wait_send()
        rows = pl.ds(t * deep, deep)
        lcopy(buf.at[1, rows, pl.ds(0, quarter)], dx_ref.at[rows], loc_dx.at[t]).wait()
    w_swap().wait_send()
    for m in range(6):
        x_msg(m).wait_send()
    for j in range(len(chunks)):
        dy_swap(j).wait_send()
        if j < 2:
            dy_direct(j, mine).wait_send()
        for m in range(6):
            for p in range(2):
                y_msg(m, j, p).wait_send()
        for t in range(2):
            out_y(t, j).wait()


def finish(last, dx_in, dw_in, tail, dx_ref, dw_ref, dx_v, dw_v, tail_v, sem_in, sem_out, sem_t):
    deep, cols = dw_in.shape
    rows = deep // PARTS
    left = cols - last
    front, back = pl.ds(0, last), pl.ds(last, left)

    def piece(i):
        if i < PARTS:
            at = pl.ds(i * rows, rows)
            return dw_in.at[at, front], dw_v.at[at, front], dw_ref.at[at, front]
        if i == PARTS:
            return dw_in.at[:, back], dw_v.at[:, back], dw_ref.at[:, back]
        return dx_in, dx_v, dx_ref

    def load(i):
        src, mid, _ = piece(i)
        return pltpu.make_async_copy(src, mid, sem_in.at[i])

    def store(i):
        _, mid, dst = piece(i)
        return pltpu.make_async_copy(mid, dst, sem_out.at[i])

    tails = pltpu.make_async_copy(tail.at[:, :, :, back], tail_v, sem_t)
    order = (*range(PARTS), PARTS + 1, PARTS)
    tails.start()
    for i in (PARTS, *range(PARTS), PARTS + 1):
        load(i).start()
    for i in order:
        load(i).wait()
        if i == PARTS:
            tails.wait()
            for t in range(2):
                at = slice(t * (deep // 2), (t + 1) * (deep // 2))
                dw_v[at, last:] += tail_v[t, 0] + tail_v[t, 1]
        store(i).start()
    for i in order:
        store(i).wait()


PARTS = 8


def solution(mesh):
    act_spec = P(("pod", "data", "row"), "col")
    wgt_spec = P(("pod", "row"), "col")
    nd, nc = mesh.shape["data"], mesh.shape["col"]

    def local_step(x_blk, w_blk, dy_blk):
        tokens, feats = x_blk.shape
        cols = dy_blk.shape[1]
        deep = w_blk.shape[0] * 2 // nd // 2
        half = deep // 2
        count = len(split(cols))
        any_spec = pl.BlockSpec(memory_space=pl.ANY)
        dma = pltpu.SemaphoreType.DMA
        outs = pl.pallas_call(
            functools.partial(kernel, nd, nc),
            out_shape=(
                jax.ShapeDtypeStruct((tokens, feats), BF16),
                jax.ShapeDtypeStruct((deep, cols), F32),
                jax.ShapeDtypeStruct((tokens, cols), BF16),
                jax.ShapeDtypeStruct(w_blk.shape, BF16),
                jax.ShapeDtypeStruct((2, 2, half, cols), F32),
            ),
            in_specs=[any_spec] * 3,
            out_specs=(any_spec,) * 5,
            scratch_shapes=[
                pltpu.VMEM((tokens, feats), BF16),
                pltpu.VMEM((feats, tokens), BF16),
                pltpu.VMEM((8, half, 2 * tokens), BF16),
                pltpu.VMEM((4, 2, half, cols), F32),
                pltpu.VMEM((2, half, cols), F32),
                pltpu.VMEM((4, 2, tokens // 2, feats), F32),
                pltpu.VMEM((2, tokens // 2, feats), F32),
                pltpu.VMEM((2, 2, tokens // 2, feats), F32),
                pltpu.VMEM((2, 2 * tokens, WIDE), BF16),
                pltpu.VMEM((2, 2, half, WIDE), F32),
                dma((2, 2, 2, 2)), dma((8, 2, 2)), dma((2,)), dma((2, 2)), dma(()),
                dma((count,)), dma((count,)), dma((2,)), dma((2,)), dma(()), dma(()), dma((2, 2)),
                dma((6, count, 2)), dma((6, count, 2)), dma((6,)), dma((6,)),
                dma((2, 2)), dma((2, count)), dma((2, 3)), dma((2,)),
            ],
            compiler_params=pltpu.CompilerParams(
                collective_id=0, has_side_effects=True, vmem_limit_bytes=67043328),
        )(x_blk, w_blk, dy_blk)
        last = split(cols)[-1][0]
        return pl.pallas_call(
            functools.partial(finish, last),
            out_shape=(
                jax.ShapeDtypeStruct((tokens, feats), BF16),
                jax.ShapeDtypeStruct((deep, cols), F32),
            ),
            in_specs=[any_spec] * 3,
            out_specs=(any_spec,) * 2,
            scratch_shapes=[
                pltpu.VMEM((tokens, feats), BF16),
                pltpu.VMEM((deep, cols), F32),
                pltpu.VMEM((2, 2, half, cols - last), F32),
                dma((PARTS + 2,)), dma((PARTS + 2,)), dma(()),
            ],
            compiler_params=pltpu.CompilerParams(vmem_limit_bytes=67043328),
        )(outs[0], outs[1], outs[4])

    return jax.shard_map(local_step, mesh=mesh, in_specs=(act_spec, wgt_spec, act_spec),
                         out_specs=(act_spec, act_spec), check_vma=False)
```

```python
import functools

import jax
import jax.numpy as jnp
from jax import lax
from jax.experimental import pallas as pl
from jax.experimental.pallas import tpu as pltpu
from jax.sharding import PartitionSpec as P

MESH = pl.DeviceIdType.MESH
F32, BF16 = jnp.float32, jnp.bfloat16

TILE = 256
DEPTH = 512
PARTS = 8


def pieces(width):
    return [(lo, min(DEPTH, width - lo)) for lo in range(0, width, DEPTH)]


def kernel(nd, nc, x_ref, w_ref, dy_ref, dx_ref, dw_ref, dyo, wo, nbr,
           xl, xs, xt, part, own, relay_y, tail_y, acc, relay_x, tail_x, buf,
           sem_p, sem_g, sem_r, rem_g, sem_h, rem_h, sem_f, loc_x, sem_a, rem_a, sem_w, rem_w,
           sem_n, rem_n, sem_s, rem_s, loc_d, loc_n, sem_y, rem_y, sem_x, rem_x, loc_o, loc_w, loc_dx):
    d, c, r = lax.axis_index("data"), lax.axis_index("col"), lax.axis_index("row")
    tokens, cols = dy_ref.shape
    band = xt.shape[2]
    span = own.shape[2]
    d_up, d_dn = (d + 1) % nd, (d + nd - 1) % nd
    c_up, c_dn = (c + 1) % nc, (c + nc - 1) % nc
    other = 1 - r
    mine = pl.ds(pl.multiple_of(r * tokens, tokens), tokens)
    theirs = pl.ds(pl.multiple_of(other * tokens, tokens), tokens)
    subs = pieces(span)
    n = len(subs)

    def rcopy(src, dst, send, recv, **to):
        return pltpu.make_async_remote_copy(src_ref=src, dst_ref=dst, send_sem=send, recv_sem=recv,
                                            device_id=to, device_id_type=MESH)

    def lcopy(src, dst, sem):
        return pltpu.make_async_copy(src, dst, sem)

    def near(k):
        return (k + c - d + nd) % nd

    def start_of(e):
        k = (d + e) % nd
        return k * span - k // (nd - 1) * (nd * span - cols)

    def cut(e, j):
        lo, w = subs[j]
        return pl.ds(pl.multiple_of(start_of(e) + lo, 128), w)

    def rows_for(core):
        return xs.at[pl.ds(pl.multiple_of(core * band, band), band)]

    def x_partner():
        return rcopy(rows_for(other), xt.at[0, 0, :, mine], sem_p, rem_g.at[0, 0, r], row=other)

    def x_side(up, core):
        k = 3 if up else 1
        return rcopy(rows_for(core), xt.at[0, k, :, mine], sem_g.at[up, core], rem_g.at[0, k, r],
                     col=c_up if up else c_dn, row=core)

    def x_rows(up, core):
        row = 2 if up else 1
        return rcopy(rows_for(core), xt.at[row, 0, :, mine], sem_r.at[up, core], rem_g.at[row, 0, r],
                     data=d_up if up else d_dn, row=core)

    def x_next(row, up):
        return rcopy(xt.at[row, 0], xt.at[row, 3 if up else 1], sem_h.at[row - 1, up], rem_h.at[row - 1, up],
                     col=c_up if up else c_dn)

    def x_pass(row, up):
        who = 0 if up else 1
        at = pl.ds(who * tokens, tokens)
        return rcopy(xt.at[row, 3 if up else 1, :, at], xt.at[row, 2, :, at], sem_f.at[row, up], rem_g.at[row, 2, who],
                     col=c_up if up else c_dn)

    def x_arrived(row, k, who):
        at = xt.at[row, k, :, pl.ds(pl.multiple_of(who * tokens, tokens), tokens)]
        return rcopy(at, at, sem_p, rem_g.at[row, k, who], row=other)

    def dy_swap():
        return rcopy(dy_ref, dyo, sem_a, rem_a, row=other)

    soon = cols // DEPTH * 2 // 5
    halves = ((0, soon * DEPTH), (soon * DEPTH, cols - soon * DEPTH))

    def w_swap(i):
        at = pl.ds(*halves[i])
        return rcopy(w_ref.at[:, at], wo.at[:, at], sem_w.at[i], rem_w.at[i], row=other)

    def dy_give(down, j):
        return rcopy(dy_ref.at[:, cut(down, j)], nbr.at[down, mine, pl.ds(*subs[j])], sem_n.at[down, j], rem_n.at[down, j],
                     data=d_dn if down else d_up)

    def dy_share(i, j, rows):
        at = nbr.at[i, rows, pl.ds(*subs[j])]
        return rcopy(at, at, sem_s.at[i, j], rem_s.at[i, j], row=other)

    def y_msg(m, j):
        at = pl.ds(*subs[j])
        i, k = ((0, 2), (1, 2), (0, 1), (1, 3), (1, 1), (0, 3))[m]
        down = m % 2
        dst = relay_y.at[down, :, at] if m < 2 else tail_y.at[(1, 0, 3, 2)[m - 2], :, at]
        return rcopy(part.at[i, k, :, at], dst, sem_y.at[m, j], rem_y.at[m, j], data=d_dn if down else d_up)

    def x_msg(m):
        k, t = ((2, 1), (2, 0), (1, 0), (3, 1), (1, 1), (3, 0))[m]
        down = m % 2
        dst = relay_x.at[down] if m < 2 else tail_x.at[t, down]
        return rcopy(acc.at[k, t], dst, sem_x.at[m], rem_x.at[m], col=c_dn if down else c_up)

    x_load = lcopy(x_ref, xl, loc_x)
    x_load.start()
    barrier = pltpu.get_barrier_semaphore()
    peers = [dict(row=other)]
    peers += [dict(data=k, row=core) for k in (d_up, d_dn) for core in range(2)]
    peers += [dict(col=k, row=core) for k in (c_up, c_dn) for core in range(2)]
    for peer in peers:
        pl.semaphore_signal(barrier, inc=1, device_id=peer, device_id_type=MESH)
    x_load.wait()
    for b in range(xl.shape[1] // 128):
        xs[b * 128:(b + 1) * 128, :] = xl[:, b * 128:(b + 1) * 128].T
    xt[0, 0, :, mine] = xs[pl.ds(pl.multiple_of(r * band, band), band), :]
    pl.semaphore_wait(barrier, len(peers))

    for core in range(2):
        for up in range(2):
            x_rows(up, core).start()
            x_side(up, core).start()
    x_partner().start()
    w_swap(0).start()
    for j in range(n):
        for down in range(2):
            dy_give(down, j).start()
    w_swap(1).start()
    dy_swap().start()

    steps = cols // DEPTH
    rest = cols - steps * DEPTH
    quarter = acc.shape[3]
    deep = acc.shape[2]

    def dx_loads(slot, lo, w):
        at, to = pl.ds(lo, w), pl.ds(pl.multiple_of(slot * DEPTH, DEPTH), w)
        return (lcopy(w_ref.at[:, at], buf.at[0, mine, to], loc_w.at[slot, 0]),
                lcopy(wo.at[:, at], buf.at[0, theirs, to], loc_w.at[slot, 1]),
                lcopy(dy_ref.at[:, at], buf.at[1, pl.ds(0, tokens), to], loc_w.at[slot, 2]))

    def dx_product(slot, w, fresh):
        to = pl.ds(pl.multiple_of(slot * DEPTH, DEPTH), w)

        def step(b, _):
            k, h = b // 2, b % 2
            rows = pl.multiple_of((c + k) % nc * quarter + h * TILE, TILE)
            at = pl.ds(pl.multiple_of(h * TILE, TILE), TILE)
            for t in range(2):
                out = lax.dot_general(buf[1, t * deep:(t + 1) * deep, to], buf[0, pl.ds(rows, TILE), to],
                                      (((1,), (1,)), ((), ())), preferred_element_type=F32)
                if fresh:
                    acc[k, t, :, at] = out
                else:
                    acc[k, t, :, at] += out
            return 0

        lax.fori_loop(0, nc * quarter // TILE, step, 0)

    def dx_run(first, stop, fresh):
        def loads(i):
            return dx_loads(i % 2, pl.multiple_of(i * DEPTH, 128), DEPTH)

        def step(i, clear):
            @pl.when(i + 1 < stop)
            def _():
                for copy in loads(i + 1):
                    copy.start()

            for copy in loads(i):
                copy.wait()
            dx_product(i % 2, DEPTH, clear)

        def body(i, _):
            step(i, False)
            return 0

        for copy in loads(first):
            copy.start()
        if fresh:
            step(jnp.int32(first), True)
        lax.fori_loop(first + fresh, stop, body, 0)

    w_swap(0).wait_recv()
    dx_run(0, soon, 1)
    for k in (1, 3):
        for who in range(2):
            x_arrived(0, k, who).wait_recv()
    for up in range(2):
        x_pass(0, up).start()
    for row in (1, 2):
        for who in range(2):
            x_arrived(row, 0, who).wait_recv()
        for up in range(2):
            x_next(row, up).start()
    w_swap(1).wait_recv()
    dx_run(soon, steps, 0)
    for copy in dx_loads(0, steps * DEPTH, rest):
        copy.start()
    for copy in dx_loads(0, steps * DEPTH, rest):
        copy.wait()
    dx_product(0, rest, False)

    def tiles(w, one):
        def step(b, _):
            one(pl.multiple_of(b * TILE, TILE), TILE)
            return 0

        lax.fori_loop(0, w // TILE, step, 0)
        if w % TILE:
            one(w - w % TILE, w % TILE)

    def dot(lhs, slot, at, width):
        return lax.dot_general(lhs, buf[slot, :, pl.ds(at, width)], (((1,), (0,)), ((), ())), preferred_element_type=F32)

    def heavy(i, j, slot):
        lo, w = subs[j]

        def one(at, width):
            to = pl.ds(pl.multiple_of(lo + at, 128), width)
            for k in (0, 2):
                out = dot(xt[0, k:k + 2].reshape(2 * band, 2 * tokens), slot, at, width)
                part[i, near(k), :, to] = out[:band]
                part[i, near(k + 1), :, to] = out[band:]

        tiles(w, one)

    def light(e, j, slot):
        lo, w = subs[j]

        def one(at, width):
            own[e, :, pl.ds(pl.multiple_of(lo + at, 128), width)] = dot(xt[0, (d - c + nc) % nc], slot, at, width)

        tiles(w, one)

    def own_load(e, j, slot):
        to = pl.ds(0, subs[j][1])
        return (lcopy(dy_ref.at[:, cut(e, j)], buf.at[slot, mine, to], loc_d.at[slot, 0]),
                lcopy(dyo.at[:, cut(e, j)], buf.at[slot, theirs, to], loc_d.at[slot, 1]))

    dy_swap().wait_recv()
    work = [(e, j) for j in range(n) for e in (3, 2)] + [(e, j) for j in range(n) for e in (0, 1)]
    for copy in own_load(*work[0], 0):
        copy.start()
    x_arrived(0, 0, other).wait_recv()
    for who in range(2):
        x_arrived(0, 2, who).wait_recv()
    for i, (e, j) in enumerate(work):
        if i + 1 < len(work):
            for copy in own_load(*work[i + 1], (i + 1) % 2):
                copy.start()
        for copy in own_load(e, j, i % 2):
            copy.wait()
        if e > 1:
            heavy(3 - e, j, i % 2)
        else:
            light(e, j, i % 2)
        if i == n:
            for up in range(2):
                x_next(1, up).wait_recv()
                x_pass(1, up).start()
        if i >= 2 * n and i % 2 and i // 2 - n < n - 1:
            for side in range(2):
                dy_give(side, i // 2 - n).wait_recv()
                dy_share(side, i // 2 - n, mine).start()

    def nbr_load(side, j, slot):
        to = pl.ds(0, subs[j][1])
        return lcopy(nbr.at[side, :, pl.ds(*subs[j])], buf.at[slot, :, to], loc_n.at[slot])

    def add(side, j, slot, ks):
        lo, w = subs[j]
        for k in ks:
            @pl.when(near(k) != (1 if side else 3))
            def _(k=k):
                def one(at, width):
                    to = pl.ds(pl.multiple_of(lo + at, 128), width)
                    part[side, near(k), :, to] += dot(xt[1 if side else 2, k], slot, at, width)

                tiles(w, one)

            for q, m in ((2, side), (3 if side else 1, 2 + side)):
                @pl.when(near(k) == q)
                def _(m=m):
                    y_msg(m, j).start()

    work = [(side, j) for j in range(n) for side in (1, 0)]
    work = [(*item, (0, 3, 1)) for item in work] + [(*item, (2,)) for item in work]
    shared = set()

    def ready(side, j):
        if (side, j) not in shared:
            shared.add((side, j))
            if j == n - 1:
                dy_give(side, j).wait_recv()
                dy_share(side, j, mine).start()
            dy_share(side, j, theirs).wait_recv()

    ready(*work[0][:2])
    nbr_load(*work[0][:2], 0).start()
    for i, (side, j, ks) in enumerate(work):
        if i + 1 < len(work):
            ready(*work[i + 1][:2])
            nbr_load(*work[i + 1][:2], (i + 1) % 2).start()
        nbr_load(side, j, i % 2).wait()
        if i == 1:
            for up in range(2):
                x_next(2, up).wait_recv()
                x_pass(2, up).start()
            for m in range(4):
                x_msg(m).start()
        if i == 2 * n:
            for row in (1, 2):
                for who in range(2):
                    x_arrived(row, 2, who).wait_recv()
        add(side, j, i % 2, ks)

    def pass_y(j):
        at = pl.ds(*subs[j])
        for down, i, k in ((0, 1, 1), (1, 0, 3)):
            y_msg(down, j).wait_recv()
            part[i, k, :, at] += relay_y[down, :, at]
            y_msg(4 + down, j).start()

    def pass_x():
        for down, k, t in ((0, 1, 1), (1, 3, 0)):
            x_msg(down).wait_recv()
            acc[k, t] += relay_x[down]
            x_msg(4 + down).start()

    pass_y(0)
    pass_x()
    for j in range(1, n):
        pass_y(j)

    def mine_of(e):
        return own.at[e] if e < 2 else part.at[3 - e, 0]

    def out_y(e, j):
        return lcopy(mine_of(e).at[:, pl.ds(*subs[j])], dw_ref.at[:, cut(e, j)], loc_o.at[e % 2])

    def done_y(pair):
        for j in range(n):
            at = pl.ds(*subs[j])
            for e in pair:
                y_msg((5, 4, 2, 3)[e], j).wait_recv()
                mine_of(e)[:, at] += tail_y[(2, 3, 1, 0)[e], :, at]
            if j:
                for e in pair:
                    out_y(e, j - 1).wait()
            for e in pair:
                out_y(e, j).start()
        for e in pair:
            out_y(e, n - 1).wait()

    done_y((3, 2))
    for t in range(2):
        for m in ((2, 5) if t == 0 else (3, 4)):
            x_msg(m).wait_recv()
        rows = pl.ds(t * deep, deep)
        buf[1, rows, 0:quarter] = (acc[0, t] + tail_x[t, 0] + tail_x[t, 1]).astype(BF16)
        lcopy(buf.at[1, rows, pl.ds(0, quarter)], dx_ref.at[rows], loc_dx.at[t]).start()
    done_y((0, 1))

    x_partner().wait_send()
    for up in range(2):
        for core in range(2):
            x_side(up, core).wait_send()
            x_rows(up, core).wait_send()
        for row in range(3):
            x_pass(row, up).wait_send()
        for row in (1, 2):
            x_next(row, up).wait_send()
    for t in range(2):
        rows = pl.ds(t * deep, deep)
        lcopy(buf.at[1, rows, pl.ds(0, quarter)], dx_ref.at[rows], loc_dx.at[t]).wait()
        w_swap(t).wait_send()
    dy_swap().wait_send()
    for m in range(6):
        x_msg(m).wait_send()
    for j in range(n):
        for side in range(2):
            dy_give(side, j).wait_send()
            dy_share(side, j, mine).wait_send()
        for m in range(6):
            y_msg(m, j).wait_send()


def finish(dx_in, dw_in, dx_ref, dw_ref, dx_v, dw_v, sem_in, sem_out):
    rows = dw_in.shape[0] // PARTS

    def piece(i):
        if i < PARTS:
            at = pl.ds(i * rows, rows)
            return dw_in.at[at], dw_v.at[at], dw_ref.at[at]
        return dx_in, dx_v, dx_ref

    def load(i):
        return pltpu.make_async_copy(*piece(i)[:2], sem_in.at[i])

    def store(i):
        return pltpu.make_async_copy(*piece(i)[1:], sem_out.at[i])

    for i in range(PARTS + 1):
        load(i).start()
    for i in range(PARTS + 1):
        load(i).wait()
        store(i).start()
    for i in range(PARTS + 1):
        store(i).wait()


def solution(mesh):
    act_spec = P(("pod", "data", "row"), "col")
    wgt_spec = P(("pod", "row"), "col")
    nd, nc, nr = mesh.shape["data"], mesh.shape["col"], mesh.shape["row"]

    def local_step(x_blk, w_blk, dy_blk):
        tokens, feats = x_blk.shape
        cols = dy_blk.shape[1]
        band = feats // nr
        span = pl.cdiv(cols, 128 * nd) * 128
        n = len(pieces(span))
        any_spec = pl.BlockSpec(memory_space=pl.ANY)
        dma = pltpu.SemaphoreType.DMA
        outs = pl.pallas_call(
            functools.partial(kernel, nd, nc),
            out_shape=(
                jax.ShapeDtypeStruct((tokens, feats), BF16),
                jax.ShapeDtypeStruct((band, cols), F32),
                jax.ShapeDtypeStruct((tokens, cols), BF16),
                jax.ShapeDtypeStruct(w_blk.shape, BF16),
                jax.ShapeDtypeStruct((2, 2 * tokens, span), BF16),
            ),
            in_specs=[any_spec] * 3,
            out_specs=(any_spec,) * 5,
            scratch_shapes=[
                pltpu.VMEM((tokens, feats), BF16),
                pltpu.VMEM((feats, tokens), BF16),
                pltpu.VMEM((3, 4, band, 2 * tokens), BF16),
                pltpu.VMEM((2, 4, band, span), F32),
                pltpu.VMEM((2, band, span), F32),
                pltpu.VMEM((2, band, span), F32),
                pltpu.VMEM((4, band, span), F32),
                pltpu.VMEM((4, 2, tokens // 2, feats), F32),
                pltpu.VMEM((2, tokens // 2, feats), F32),
                pltpu.VMEM((2, 2, tokens // 2, feats), F32),
                pltpu.VMEM((2, 2 * tokens, 2 * DEPTH), BF16),
                dma(()), dma((2, 2)), dma((2, 2)), dma((3, 4, 2)), dma((2, 2)), dma((2, 2)), dma((3, 2)), dma(()),
                dma(()), dma(()), dma((2,)), dma((2,)),
                dma((2, n)), dma((2, n)), dma((2, n)), dma((2, n)), dma((2, 2)), dma((2,)),
                dma((6, n)), dma((6, n)), dma((6,)), dma((6,)), dma((2,)), dma((2, 3)), dma((2,)),
            ],
            compiler_params=pltpu.CompilerParams(
                collective_id=0, has_side_effects=True, vmem_limit_bytes=67043328),
        )(x_blk, w_blk, dy_blk)
        return pl.pallas_call(
            finish,
            out_shape=(
                jax.ShapeDtypeStruct((tokens, feats), BF16),
                jax.ShapeDtypeStruct((band, cols), F32),
            ),
            in_specs=[any_spec] * 2,
            out_specs=(any_spec,) * 2,
            scratch_shapes=[
                pltpu.VMEM((tokens, feats), BF16),
                pltpu.VMEM((band, cols), F32),
                dma((PARTS + 1,)), dma((PARTS + 1,)),
            ],
            compiler_params=pltpu.CompilerParams(vmem_limit_bytes=67043328),
        )(outs[0], outs[1])

    return jax.shard_map(local_step, mesh=mesh, in_specs=(act_spec, wgt_spec, act_spec),
                         out_specs=(act_spec, act_spec), check_vma=False)
```

```python
import functools

import jax
import jax.numpy as jnp
from jax import lax
from jax.experimental import pallas as pl
from jax.experimental.pallas import tpu as pltpu
from jax.sharding import PartitionSpec as P

MESH = pl.DeviceIdType.MESH
F32, BF16 = jnp.float32, jnp.bfloat16

TILE = 256
DEPTH = 512
PARTS = 8


def pieces(width):
    return [(lo, min(DEPTH, width - lo)) for lo in range(0, width, DEPTH)]


def kernel(nd, nc, x_ref, w_ref, dy_ref, dx_ref, dw_ref, dyo, wo, nbr,
           xl, xs, xt, part, own, relay_y, tail_y, acc, relay_x, tail_x, buf,
           sem_p, sem_g, sem_r, rem_g, sem_h, rem_h, sem_f, loc_x, sem_a, rem_a, sem_w, rem_w,
           sem_n, rem_n, sem_s, rem_s, loc_d, loc_n, sem_y, rem_y, sem_x, rem_x, loc_o, loc_w, loc_dx):
    d, c, r = lax.axis_index("data"), lax.axis_index("col"), lax.axis_index("row")
    tokens, cols = dy_ref.shape
    band = xt.shape[2]
    span = own.shape[2]
    d_up, d_dn = (d + 1) % nd, (d + nd - 1) % nd
    c_up, c_dn = (c + 1) % nc, (c + nc - 1) % nc
    other = 1 - r
    mine = pl.ds(pl.multiple_of(r * tokens, tokens), tokens)
    theirs = pl.ds(pl.multiple_of(other * tokens, tokens), tokens)
    subs = pieces(span)
    n = len(subs)

    def rcopy(src, dst, send, recv, **to):
        return pltpu.make_async_remote_copy(src_ref=src, dst_ref=dst, send_sem=send, recv_sem=recv,
                                            device_id=to, device_id_type=MESH)

    def lcopy(src, dst, sem):
        return pltpu.make_async_copy(src, dst, sem)

    def near(k):
        return (k + c - d + nd) % nd

    def used(row, k):
        return near(k) != (1 if row == 1 else 3)

    def start_of(e):
        k = (d + e) % nd
        return k * span - k // (nd - 1) * (nd * span - cols)

    def cut(e, j):
        lo, w = subs[j]
        return pl.ds(pl.multiple_of(start_of(e) + lo, 128), w)

    def rows_for(core):
        return xs.at[pl.ds(pl.multiple_of(core * band, band), band)]

    def x_partner():
        return rcopy(rows_for(other), xt.at[0, 0, :, mine], sem_p, rem_g.at[0, 0, r], row=other)

    def x_side(up, core):
        k = 3 if up else 1
        return rcopy(rows_for(core), xt.at[0, k, :, mine], sem_g.at[up, core], rem_g.at[0, k, r],
                     col=c_up if up else c_dn, row=core)

    def x_rows(up, core):
        row = 2 if up else 1
        return rcopy(rows_for(core), xt.at[row, 0, :, mine], sem_r.at[up, core], rem_g.at[row, 0, r],
                     data=d_up if up else d_dn, row=core)

    def x_next(row, up):
        return rcopy(xt.at[row, 0], xt.at[row, 3 if up else 1], sem_h.at[row - 1, up], rem_h.at[row - 1, up],
                     col=c_up if up else c_dn)

    def x_pass(row, up):
        who = 0 if up else 1
        at = pl.ds(who * tokens, tokens)
        return rcopy(xt.at[row, 3 if up else 1, :, at], xt.at[row, 2, :, at], sem_f.at[row, up], rem_g.at[row, 2, who],
                     col=c_up if up else c_dn)

    def x_arrived(row, k, who):
        at = xt.at[row, k, :, pl.ds(pl.multiple_of(who * tokens, tokens), tokens)]
        return rcopy(at, at, sem_p, rem_g.at[row, k, who], row=other)

    def dy_swap():
        return rcopy(dy_ref, dyo, sem_a, rem_a, row=other)

    soon = cols // DEPTH * 2 // 5
    halves = ((0, soon * DEPTH), (soon * DEPTH, cols - soon * DEPTH))

    def w_swap(i):
        at = pl.ds(*halves[i])
        return rcopy(w_ref.at[:, at], wo.at[:, at], sem_w.at[i], rem_w.at[i], row=other)

    def dy_give(down, j):
        return rcopy(dy_ref.at[:, cut(down, j)], nbr.at[down, mine, pl.ds(*subs[j])], sem_n.at[down, j], rem_n.at[down, j],
                     data=d_dn if down else d_up)

    def dy_share(i, j, rows):
        at = nbr.at[i, rows, pl.ds(*subs[j])]
        return rcopy(at, at, sem_s.at[i, j], rem_s.at[i, j], row=other)

    def y_msg(m, j):
        at = pl.ds(*subs[j])
        i, k = ((0, 2), (1, 2), (0, 1), (1, 3), (1, 1), (0, 3))[m]
        down = m % 2
        dst = relay_y.at[down, :, at] if m < 2 else tail_y.at[(1, 0, 3, 2)[m - 2], :, at]
        return rcopy(part.at[i, k, :, at], dst, sem_y.at[m, j], rem_y.at[m, j], data=d_dn if down else d_up)

    def x_msg(m):
        k, t = ((2, 1), (2, 0), (1, 0), (3, 1), (1, 1), (3, 0))[m]
        down = m % 2
        dst = relay_x.at[down] if m < 2 else tail_x.at[t, down]
        return rcopy(acc.at[k, t], dst, sem_x.at[m], rem_x.at[m], col=c_dn if down else c_up)

    x_load = lcopy(x_ref, xl, loc_x)
    x_load.start()
    barrier = pltpu.get_barrier_semaphore()
    peers = [dict(row=other)]
    peers += [dict(data=k, row=core) for k in (d_up, d_dn) for core in range(2)]
    peers += [dict(col=k, row=core) for k in (c_up, c_dn) for core in range(2)]
    for peer in peers:
        pl.semaphore_signal(barrier, inc=1, device_id=peer, device_id_type=MESH)
    x_load.wait()
    for b in range(xl.shape[1] // 128):
        xs[b * 128:(b + 1) * 128, :] = xl[:, b * 128:(b + 1) * 128].T
    xt[0, 0, :, mine] = xs[pl.ds(pl.multiple_of(r * band, band), band), :]
    pl.semaphore_wait(barrier, len(peers))

    for core in range(2):
        for up in range(2):
            @pl.when(near(0) != 0)
            def _(up=up, core=core):
                x_rows(up, core).start()

            x_side(up, core).start()
    x_partner().start()
    w_swap(0).start()
    for j in range(n):
        for down in range(2):
            dy_give(down, j).start()
    w_swap(1).start()
    dy_swap().start()

    steps = cols // DEPTH
    rest = cols - steps * DEPTH
    quarter = acc.shape[3]
    deep = acc.shape[2]

    def dx_loads(slot, lo, w):
        at, to = pl.ds(lo, w), pl.ds(pl.multiple_of(slot * DEPTH, DEPTH), w)
        return (lcopy(w_ref.at[:, at], buf.at[0, mine, to], loc_w.at[slot, 0]),
                lcopy(wo.at[:, at], buf.at[0, theirs, to], loc_w.at[slot, 1]),
                lcopy(dy_ref.at[:, at], buf.at[1, pl.ds(0, tokens), to], loc_w.at[slot, 2]))

    def dx_product(slot, w, fresh):
        to = pl.ds(pl.multiple_of(slot * DEPTH, DEPTH), w)

        def step(b, _):
            k, h = b // 2, b % 2
            rows = pl.multiple_of((c + k) % nc * quarter + h * TILE, TILE)
            at = pl.ds(pl.multiple_of(h * TILE, TILE), TILE)
            for t in range(2):
                out = lax.dot_general(buf[1, t * deep:(t + 1) * deep, to], buf[0, pl.ds(rows, TILE), to],
                                      (((1,), (1,)), ((), ())), preferred_element_type=F32)
                if fresh:
                    acc[k, t, :, at] = out
                else:
                    acc[k, t, :, at] += out
            return 0

        lax.fori_loop(0, nc * quarter // TILE, step, 0)

    def dx_run(first, stop, fresh):
        def loads(i):
            return dx_loads(i % 2, pl.multiple_of(i * DEPTH, 128), DEPTH)

        def step(i, clear):
            @pl.when(i + 1 < stop)
            def _():
                for copy in loads(i + 1):
                    copy.start()

            for copy in loads(i):
                copy.wait()
            dx_product(i % 2, DEPTH, clear)

        def body(i, _):
            step(i, False)
            return 0

        for copy in loads(first):
            copy.start()
        if fresh:
            step(jnp.int32(first), True)
        lax.fori_loop(first + fresh, stop, body, 0)

    w_swap(0).wait_recv()
    dx_run(0, soon, 1)
    for k in (1, 3):
        for who in range(2):
            x_arrived(0, k, who).wait_recv()
    for up in range(2):
        x_pass(0, up).start()
    for row in (1, 2):
        @pl.when(used(row, 0))
        def _(row=row):
            for who in range(2):
                x_arrived(row, 0, who).wait_recv()
            for up in range(2):
                x_next(row, up).start()
    w_swap(1).wait_recv()
    dx_run(soon, steps, 0)
    for copy in dx_loads(0, steps * DEPTH, rest):
        copy.start()
    for copy in dx_loads(0, steps * DEPTH, rest):
        copy.wait()
    dx_product(0, rest, False)

    def tiles(w, one):
        def step(b, _):
            one(pl.multiple_of(b * TILE, TILE), TILE)
            return 0

        lax.fori_loop(0, w // TILE, step, 0)
        if w % TILE:
            one(w - w % TILE, w % TILE)

    def dot(lhs, slot, at, width):
        return lax.dot_general(lhs, buf[slot, :, pl.ds(at, width)], (((1,), (0,)), ((), ())), preferred_element_type=F32)

    def heavy(i, j, slot):
        lo, w = subs[j]

        def one(at, width):
            to = pl.ds(pl.multiple_of(lo + at, 128), width)
            for k in (0, 2):
                out = dot(xt[0, k:k + 2].reshape(2 * band, 2 * tokens), slot, at, width)
                part[i, near(k), :, to] = out[:band]
                part[i, near(k + 1), :, to] = out[band:]

        tiles(w, one)

    def light(e, j, slot):
        lo, w = subs[j]

        def one(at, width):
            own[e, :, pl.ds(pl.multiple_of(lo + at, 128), width)] = dot(xt[0, (d - c + nc) % nc], slot, at, width)

        tiles(w, one)

    def own_load(e, j, slot):
        to = pl.ds(0, subs[j][1])
        return (lcopy(dy_ref.at[:, cut(e, j)], buf.at[slot, mine, to], loc_d.at[slot, 0]),
                lcopy(dyo.at[:, cut(e, j)], buf.at[slot, theirs, to], loc_d.at[slot, 1]))

    def pass_on(row):
        for up in range(2):
            @pl.when(used(row, 3 if up else 1))
            def _(up=up):
                x_next(row, up).wait_recv()
                x_pass(row, up).start()

    dy_swap().wait_recv()
    work = [(e, j) for j in range(n) for e in (3, 2)]
    for copy in own_load(*work[0], 0):
        copy.start()
    x_arrived(0, 0, other).wait_recv()
    for who in range(2):
        x_arrived(0, 2, who).wait_recv()
    for i, (e, j) in enumerate(work):
        if i + 1 < len(work):
            for copy in own_load(*work[i + 1], (i + 1) % 2):
                copy.start()
        for copy in own_load(e, j, i % 2):
            copy.wait()
        heavy(3 - e, j, i % 2)
        if i == n:
            pass_on(1)
        if i % 2 and i // 2 < n - 1:
            for side in range(2):
                dy_give(side, i // 2).wait_recv()
                dy_share(side, i // 2, mine).start()

    def nbr_load(side, j, slot):
        to = pl.ds(0, subs[j][1])
        return lcopy(nbr.at[side, :, pl.ds(*subs[j])], buf.at[slot, :, to], loc_n.at[slot])

    def add(side, j, slot, ks):
        lo, w = subs[j]
        for k in ks:
            @pl.when(near(k) != (1 if side else 3))
            def _(k=k):
                def one(at, width):
                    to = pl.ds(pl.multiple_of(lo + at, 128), width)
                    part[side, near(k), :, to] += dot(xt[1 if side else 2, k], slot, at, width)

                tiles(w, one)

            for q, m in ((2, side), (3 if side else 1, 2 + side)):
                @pl.when(near(k) == q)
                def _(m=m):
                    y_msg(m, j).start()

    work = [(side, j) for j in range(n) for side in (1, 0)]
    shared = set()

    def ready(side, j):
        if (side, j) not in shared:
            shared.add((side, j))
            if j == n - 1:
                dy_give(side, j).wait_recv()
                dy_share(side, j, mine).start()
            dy_share(side, j, theirs).wait_recv()

    def add_all(ks, between):
        ready(*work[0])
        nbr_load(*work[0], 0).start()
        for i, (side, j) in enumerate(work):
            if i + 1 < len(work):
                ready(*work[i + 1])
                nbr_load(*work[i + 1], (i + 1) % 2).start()
            nbr_load(side, j, i % 2).wait()
            if i == 1:
                between()
            add(side, j, i % 2, ks)

    def between():
        pass_on(2)
        for m in range(4):
            x_msg(m).start()

    add_all((0, 3, 1), between)

    last = [(e, j) for j in range(n) for e in (0, 1)]
    for copy in own_load(*last[0], 0):
        copy.start()
    for i, (e, j) in enumerate(last):
        if i + 1 < len(last):
            for copy in own_load(*last[i + 1], (i + 1) % 2):
                copy.start()
        for copy in own_load(e, j, i % 2):
            copy.wait()
        light(e, j, i % 2)

    for row in (1, 2):
        @pl.when(used(row, 2))
        def _(row=row):
            for who in range(2):
                x_arrived(row, 2, who).wait_recv()
    add_all((2,), lambda: None)

    def pass_y(j):
        at = pl.ds(*subs[j])
        for down, i, k in ((0, 1, 1), (1, 0, 3)):
            y_msg(down, j).wait_recv()
            part[i, k, :, at] += relay_y[down, :, at]
            y_msg(4 + down, j).start()

    def pass_x():
        for down, k, t in ((0, 1, 1), (1, 3, 0)):
            x_msg(down).wait_recv()
            acc[k, t] += relay_x[down]
            x_msg(4 + down).start()

    pass_y(0)
    pass_x()
    for j in range(1, n):
        pass_y(j)

    def mine_of(e):
        return own.at[e] if e < 2 else part.at[3 - e, 0]

    def out_y(e, j):
        return lcopy(mine_of(e).at[:, pl.ds(*subs[j])], dw_ref.at[:, cut(e, j)], loc_o.at[e % 2])

    def done_y(pair):
        for j in range(n):
            at = pl.ds(*subs[j])
            for e in pair:
                y_msg((5, 4, 2, 3)[e], j).wait_recv()
                mine_of(e)[:, at] += tail_y[(2, 3, 1, 0)[e], :, at]
                if j:
                    out_y(e, j - 1).wait()
                out_y(e, j).start()
        for e in pair:
            out_y(e, n - 1).wait()

    done_y((3, 2))
    for t in range(2):
        for m in ((2, 5) if t == 0 else (3, 4)):
            x_msg(m).wait_recv()
        rows = pl.ds(t * deep, deep)
        buf[1, rows, 0:quarter] = (acc[0, t] + tail_x[t, 0] + tail_x[t, 1]).astype(BF16)
        lcopy(buf.at[1, rows, pl.ds(0, quarter)], dx_ref.at[rows], loc_dx.at[t]).start()
    x_partner().wait_send()
    for up in range(2):
        for core in range(2):
            x_side(up, core).wait_send()

            @pl.when(near(0) != 0)
            def _(up=up, core=core):
                x_rows(up, core).wait_send()
        x_pass(0, up).wait_send()
        for row in (1, 2):
            @pl.when(used(row, 3 if up else 1))
            def _(row=row, up=up):
                x_pass(row, up).wait_send()

            @pl.when(used(row, 0))
            def _(row=row, up=up):
                x_next(row, up).wait_send()
    for t in range(2):
        rows = pl.ds(t * deep, deep)
        lcopy(buf.at[1, rows, pl.ds(0, quarter)], dx_ref.at[rows], loc_dx.at[t]).wait()
        w_swap(t).wait_send()
    dy_swap().wait_send()
    for m in range(6):
        x_msg(m).wait_send()
    for j in range(n):
        for side in range(2):
            dy_give(side, j).wait_send()
            dy_share(side, j, mine).wait_send()
        for m in range(4):
            y_msg(m, j).wait_send()
    done_y((0, 1))
    for j in range(n):
        for m in (4, 5):
            y_msg(m, j).wait_send()


def finish(dx_in, dw_in, dx_ref, dw_ref, dx_v, dw_v, sem_in, sem_out):
    rows = dw_in.shape[0] // PARTS

    def piece(i):
        if i < PARTS:
            at = pl.ds(i * rows, rows)
            return dw_in.at[at], dw_v.at[at], dw_ref.at[at]
        return dx_in, dx_v, dx_ref

    def load(i):
        return pltpu.make_async_copy(*piece(i)[:2], sem_in.at[i])

    def store(i):
        return pltpu.make_async_copy(*piece(i)[1:], sem_out.at[i])

    for i in range(PARTS + 1):
        load(i).start()
    for i in range(PARTS + 1):
        load(i).wait()
        store(i).start()
    for i in range(PARTS + 1):
        store(i).wait()


def solution(mesh):
    act_spec = P(("pod", "data", "row"), "col")
    wgt_spec = P(("pod", "row"), "col")
    nd, nc, nr = mesh.shape["data"], mesh.shape["col"], mesh.shape["row"]

    def local_step(x_blk, w_blk, dy_blk):
        tokens, feats = x_blk.shape
        cols = dy_blk.shape[1]
        band = feats // nr
        span = pl.cdiv(cols, 128 * nd) * 128
        n = len(pieces(span))
        any_spec = pl.BlockSpec(memory_space=pl.ANY)
        dma = pltpu.SemaphoreType.DMA
        outs = pl.pallas_call(
            functools.partial(kernel, nd, nc),
            out_shape=(
                jax.ShapeDtypeStruct((tokens, feats), BF16),
                jax.ShapeDtypeStruct((band, cols), F32),
                jax.ShapeDtypeStruct((tokens, cols), BF16),
                jax.ShapeDtypeStruct(w_blk.shape, BF16),
                jax.ShapeDtypeStruct((2, 2 * tokens, span), BF16),
            ),
            in_specs=[any_spec] * 3,
            out_specs=(any_spec,) * 5,
            scratch_shapes=[
                pltpu.VMEM((tokens, feats), BF16),
                pltpu.VMEM((feats, tokens), BF16),
                pltpu.VMEM((3, 4, band, 2 * tokens), BF16),
                pltpu.VMEM((2, 4, band, span), F32),
                pltpu.VMEM((2, band, span), F32),
                pltpu.VMEM((2, band, span), F32),
                pltpu.VMEM((4, band, span), F32),
                pltpu.VMEM((4, 2, tokens // 2, feats), F32),
                pltpu.VMEM((2, tokens // 2, feats), F32),
                pltpu.VMEM((2, 2, tokens // 2, feats), F32),
                pltpu.VMEM((2, 2 * tokens, 2 * DEPTH), BF16),
                dma(()), dma((2, 2)), dma((2, 2)), dma((3, 4, 2)), dma((2, 2)), dma((2, 2)), dma((3, 2)), dma(()),
                dma(()), dma(()), dma((2,)), dma((2,)),
                dma((2, n)), dma((2, n)), dma((2, n)), dma((2, n)), dma((2, 2)), dma((2,)),
                dma((6, n)), dma((6, n)), dma((6,)), dma((6,)), dma((2,)), dma((2, 3)), dma((2,)),
            ],
            compiler_params=pltpu.CompilerParams(
                collective_id=0, has_side_effects=True, vmem_limit_bytes=67043328),
        )(x_blk, w_blk, dy_blk)
        return pl.pallas_call(
            finish,
            out_shape=(
                jax.ShapeDtypeStruct((tokens, feats), BF16),
                jax.ShapeDtypeStruct((band, cols), F32),
            ),
            in_specs=[any_spec] * 2,
            out_specs=(any_spec,) * 2,
            scratch_shapes=[
                pltpu.VMEM((tokens, feats), BF16),
                pltpu.VMEM((band, cols), F32),
                dma((PARTS + 1,)), dma((PARTS + 1,)),
            ],
            compiler_params=pltpu.CompilerParams(vmem_limit_bytes=67043328),
        )(outs[0], outs[1])

    return jax.shard_map(local_step, mesh=mesh, in_specs=(act_spec, wgt_spec, act_spec),
                         out_specs=(act_spec, act_spec), check_vma=False)
```

```python
import functools

import jax
import jax.numpy as jnp
from jax import lax
from jax.experimental import pallas as pl
from jax.experimental.pallas import tpu as pltpu
from jax.sharding import PartitionSpec as P

MESH = pl.DeviceIdType.MESH
F32, BF16 = jnp.float32, jnp.bfloat16

TILE = 256
DEPTH = 512
PARTS = 8


def pieces(width):
    return [(lo, min(DEPTH, width - lo)) for lo in range(0, width, DEPTH)]


def kernel(nd, nc, x_ref, w_ref, dy_ref, dx_ref, dw_ref, dyo, wo, nbr,
           xl, xs, xt, part, own, relay_y, tail_y, acc, relay_x, tail_x, buf,
           sem_p, sem_g, sem_r, rem_g, sem_h, rem_h, sem_f, loc_x, sem_a, rem_a, sem_w, rem_w,
           sem_n, rem_n, sem_s, rem_s, loc_d, loc_n, sem_y, rem_y, sem_x, rem_x, loc_o, loc_w, loc_dx):
    d, c, r = lax.axis_index("data"), lax.axis_index("col"), lax.axis_index("row")
    tokens, cols = dy_ref.shape
    band = xt.shape[2]
    span = own.shape[2]
    d_up, d_dn = (d + 1) % nd, (d + nd - 1) % nd
    c_up, c_dn = (c + 1) % nc, (c + nc - 1) % nc
    other = 1 - r
    mine = pl.ds(pl.multiple_of(r * tokens, tokens), tokens)
    theirs = pl.ds(pl.multiple_of(other * tokens, tokens), tokens)
    subs = pieces(span)
    n = len(subs)

    def rcopy(src, dst, send, recv, **to):
        return pltpu.make_async_remote_copy(src_ref=src, dst_ref=dst, send_sem=send, recv_sem=recv,
                                            device_id=to, device_id_type=MESH)

    def lcopy(src, dst, sem):
        return pltpu.make_async_copy(src, dst, sem)

    def near(k):
        return (k + c - d + nd) % nd

    def used(row, k):
        return near(k) != (1 if row == 1 else 3)

    def start_of(e):
        k = (d + e) % nd
        return k * span - k // (nd - 1) * (nd * span - cols)

    def cut(e, j):
        lo, w = subs[j]
        return pl.ds(pl.multiple_of(start_of(e) + lo, 128), w)

    def rows_for(core):
        return xs.at[pl.ds(pl.multiple_of(core * band, band), band)]

    def x_partner():
        return rcopy(rows_for(other), xt.at[0, 0, :, mine], sem_p, rem_g.at[0, 0, r], row=other)

    def x_side(up, core):
        k = 3 if up else 1
        return rcopy(rows_for(core), xt.at[0, k, :, mine], sem_g.at[up, core], rem_g.at[0, k, r],
                     col=c_up if up else c_dn, row=core)

    def x_rows(up, core):
        row = 2 if up else 1
        return rcopy(rows_for(core), xt.at[row, 0, :, mine], sem_r.at[up, core], rem_g.at[row, 0, r],
                     data=d_up if up else d_dn, row=core)

    def x_next(row, up):
        return rcopy(xt.at[row, 0], xt.at[row, 3 if up else 1], sem_h.at[row - 1, up], rem_h.at[row - 1, up],
                     col=c_up if up else c_dn)

    def x_pass(row, up):
        who = 0 if up else 1
        at = pl.ds(who * tokens, tokens)
        return rcopy(xt.at[row, 3 if up else 1, :, at], xt.at[row, 2, :, at], sem_f.at[row, up], rem_g.at[row, 2, who],
                     col=c_up if up else c_dn)

    def x_arrived(row, k, who):
        at = xt.at[row, k, :, pl.ds(pl.multiple_of(who * tokens, tokens), tokens)]
        return rcopy(at, at, sem_p, rem_g.at[row, k, who], row=other)

    def dy_swap():
        return rcopy(dy_ref, dyo, sem_a, rem_a, row=other)

    soon = cols // DEPTH * 3 // 10
    halves = ((0, soon * DEPTH), (soon * DEPTH, cols - soon * DEPTH))

    def w_swap(i):
        at = pl.ds(*halves[i])
        return rcopy(w_ref.at[:, at], wo.at[:, at], sem_w.at[i], rem_w.at[i], row=other)

    def dy_give(down, j):
        return rcopy(dy_ref.at[:, cut(down, j)], nbr.at[down, mine, pl.ds(*subs[j])], sem_n.at[down, j], rem_n.at[down, j],
                     data=d_dn if down else d_up)

    def dy_share(i, j, rows):
        at = nbr.at[i, rows, pl.ds(*subs[j])]
        return rcopy(at, at, sem_s.at[i, j], rem_s.at[i, j], row=other)

    def y_msg(m, j):
        at = pl.ds(*subs[j])
        i, k = ((0, 2), (1, 2), (0, 1), (1, 3), (1, 1), (0, 3))[m]
        down = m % 2
        dst = relay_y.at[down, :, at] if m < 2 else tail_y.at[(1, 0, 3, 2)[m - 2], :, at]
        return rcopy(part.at[i, k, :, at], dst, sem_y.at[m, j], rem_y.at[m, j], data=d_dn if down else d_up)

    def x_msg(m):
        k, t = ((2, 1), (2, 0), (1, 0), (3, 1), (1, 1), (3, 0))[m]
        down = m % 2
        dst = relay_x.at[down] if m < 2 else tail_x.at[t, down]
        return rcopy(acc.at[k, t], dst, sem_x.at[m], rem_x.at[m], col=c_dn if down else c_up)

    x_load = lcopy(x_ref, xl, loc_x)
    x_load.start()
    barrier = pltpu.get_barrier_semaphore()
    peers = [dict(row=other)]
    peers += [dict(data=k, row=core) for k in (d_up, d_dn) for core in range(2)]
    peers += [dict(col=k, row=core) for k in (c_up, c_dn) for core in range(2)]
    for peer in peers:
        pl.semaphore_signal(barrier, inc=1, device_id=peer, device_id_type=MESH)
    x_load.wait()
    for b in range(xl.shape[1] // 128):
        xs[b * 128:(b + 1) * 128, :] = xl[:, b * 128:(b + 1) * 128].T
    xt[0, 0, :, mine] = xs[pl.ds(pl.multiple_of(r * band, band), band), :]
    pl.semaphore_wait(barrier, len(peers))

    for core in range(2):
        for up in range(2):
            @pl.when(near(0) != 0)
            def _(up=up, core=core):
                x_rows(up, core).start()

            x_side(up, core).start()
    x_partner().start()
    w_swap(0).start()
    for j in range(n):
        for down in range(2):
            dy_give(down, j).start()
    w_swap(1).start()
    dy_swap().start()

    steps = cols // DEPTH
    rest = cols - steps * DEPTH
    quarter = acc.shape[3]
    deep = acc.shape[2]

    def dx_loads(slot, lo, w):
        at, to = pl.ds(lo, w), pl.ds(pl.multiple_of(slot * DEPTH, DEPTH), w)
        return (lcopy(w_ref.at[:, at], buf.at[0, mine, to], loc_w.at[slot, 0]),
                lcopy(wo.at[:, at], buf.at[0, theirs, to], loc_w.at[slot, 1]),
                lcopy(dy_ref.at[:, at], buf.at[1, pl.ds(0, tokens), to], loc_w.at[slot, 2]))

    def dx_product(slot, w, fresh):
        to = pl.ds(pl.multiple_of(slot * DEPTH, DEPTH), w)

        def step(b, _):
            k, h = b // 2, b % 2
            rows = pl.multiple_of((c + k) % nc * quarter + h * TILE, TILE)
            at = pl.ds(pl.multiple_of(h * TILE, TILE), TILE)
            for t in range(2):
                out = lax.dot_general(buf[1, t * deep:(t + 1) * deep, to], buf[0, pl.ds(rows, TILE), to],
                                      (((1,), (1,)), ((), ())), preferred_element_type=F32)
                if fresh:
                    acc[k, t, :, at] = out
                else:
                    acc[k, t, :, at] += out
            return 0

        lax.fori_loop(0, nc * quarter // TILE, step, 0)

    def dx_run(first, stop, fresh):
        def loads(i):
            return dx_loads(i % 2, pl.multiple_of(i * DEPTH, 128), DEPTH)

        def step(i, clear):
            @pl.when(i + 1 < stop)
            def _():
                for copy in loads(i + 1):
                    copy.start()

            for copy in loads(i):
                copy.wait()
            dx_product(i % 2, DEPTH, clear)

        def body(i, _):
            step(i, False)
            return 0

        for copy in loads(first):
            copy.start()
        if fresh:
            step(jnp.int32(first), True)
        lax.fori_loop(first + fresh, stop, body, 0)

    w_swap(0).wait_recv()
    dx_run(0, soon, 1)
    for k in (1, 3):
        for who in range(2):
            x_arrived(0, k, who).wait_recv()
    for up in range(2):
        x_pass(0, up).start()
    for row in (1, 2):
        @pl.when(used(row, 0))
        def _(row=row):
            for who in range(2):
                x_arrived(row, 0, who).wait_recv()
            for up in range(2):
                x_next(row, up).start()
    w_swap(1).wait_recv()
    dx_run(soon, steps, 0)
    for copy in dx_loads(0, steps * DEPTH, rest):
        copy.start()
    for copy in dx_loads(0, steps * DEPTH, rest):
        copy.wait()
    dx_product(0, rest, False)

    def tiles(w, one):
        def step(b, _):
            one(pl.multiple_of(b * TILE, TILE), TILE)
            return 0

        lax.fori_loop(0, w // TILE, step, 0)
        if w % TILE:
            one(w - w % TILE, w % TILE)

    def dot(lhs, slot, at, width):
        return lax.dot_general(lhs, buf[slot, :, pl.ds(at, width)], (((1,), (0,)), ((), ())), preferred_element_type=F32)

    def heavy(i, j, slot):
        lo, w = subs[j]

        def one(at, width):
            to = pl.ds(pl.multiple_of(lo + at, 128), width)
            for k in (0, 2):
                out = dot(xt[0, k:k + 2].reshape(2 * band, 2 * tokens), slot, at, width)
                part[i, near(k), :, to] = out[:band]
                part[i, near(k + 1), :, to] = out[band:]

        tiles(w, one)

    def light(e, j, slot):
        lo, w = subs[j]

        def one(at, width):
            own[e, :, pl.ds(pl.multiple_of(lo + at, 128), width)] = dot(xt[0, (d - c + nc) % nc], slot, at, width)

        tiles(w, one)

    def own_load(e, j, slot):
        to = pl.ds(0, subs[j][1])
        return (lcopy(dy_ref.at[:, cut(e, j)], buf.at[slot, mine, to], loc_d.at[slot, 0]),
                lcopy(dyo.at[:, cut(e, j)], buf.at[slot, theirs, to], loc_d.at[slot, 1]))

    def pass_on(row):
        for up in range(2):
            @pl.when(used(row, 3 if up else 1))
            def _(up=up):
                x_next(row, up).wait_recv()
                x_pass(row, up).start()

    def nbr_load(side, j, slot):
        to = pl.ds(0, subs[j][1])
        return lcopy(nbr.at[side, :, pl.ds(*subs[j])], buf.at[slot, :, to], loc_n.at[slot])

    def add(side, j, slot, ks):
        lo, w = subs[j]
        for k in ks:
            @pl.when(near(k) != (1 if side else 3))
            def _(k=k):
                def one(at, width):
                    to = pl.ds(pl.multiple_of(lo + at, 128), width)
                    part[side, near(k), :, to] += dot(xt[1 if side else 2, k], slot, at, width)

                tiles(w, one)

            for q, m in ((2, side), (3 if side else 1, 2 + side)):
                @pl.when(near(k) == q)
                def _(m=m):
                    y_msg(m, j).start()

    shared = set()

    def ready(side, j):
        if (side, j) not in shared:
            shared.add((side, j))
            if j == n - 1:
                dy_give(side, j).wait_recv()
                dy_share(side, j, mine).start()
            dy_share(side, j, theirs).wait_recv()

    def heavies(j):
        return [(True, e, j) for e in (3, 2)]

    def adds(j):
        return [(False, side, j) for side in (1, 0)]

    def run(work, ks, before):
        def load(i):
            own_tokens, e, j = work[i]
            if own_tokens:
                return own_load(e, j, i % 2)
            ready(e, j)
            return (nbr_load(e, j, i % 2),)

        def wait(i):
            own_tokens, e, j = work[i]
            for copy in own_load(e, j, i % 2) if own_tokens else (nbr_load(e, j, i % 2),):
                copy.wait()

        for copy in load(0):
            copy.start()
        for i, (own_tokens, e, j) in enumerate(work):
            before(i)
            if i + 1 < len(work):
                for copy in load(i + 1):
                    copy.start()
            wait(i)
            if own_tokens:
                heavy(3 - e, j, i % 2)
            else:
                add(e, j, i % 2, ks)

    work = [item for j in range(n - 1) for item in heavies(j)] + adds(0) + heavies(n - 1)
    first = 2 * n - 2
    work += [item for j in range(1, n) for item in adds(j)]

    def share(j):
        for side in range(2):
            dy_give(side, j).wait_recv()
            dy_share(side, j, mine).start()

    def before(i):
        if i == first - 1:
            share(0)
            pass_on(1)
        if i == first + 1:
            pass_on(2)
            for m in range(4):
                x_msg(m).start()
        if i == first + 2:
            for j in range(1, n - 1):
                share(j)

    dy_swap().wait_recv()
    x_arrived(0, 0, other).wait_recv()
    for who in range(2):
        x_arrived(0, 2, who).wait_recv()
    run(work, (0, 3, 1), before)

    last = [(e, j) for j in range(n) for e in (0, 1)]
    for copy in own_load(*last[0], 0):
        copy.start()
    for i, (e, j) in enumerate(last):
        if i + 1 < len(last):
            for copy in own_load(*last[i + 1], (i + 1) % 2):
                copy.start()
        for copy in own_load(e, j, i % 2):
            copy.wait()
        light(e, j, i % 2)

    for row in (1, 2):
        @pl.when(used(row, 2))
        def _(row=row):
            for who in range(2):
                x_arrived(row, 2, who).wait_recv()
    run([item for j in range(n) for item in adds(j)], (2,), lambda i: None)

    def pass_y(j):
        at = pl.ds(*subs[j])
        for down, i, k in ((0, 1, 1), (1, 0, 3)):
            y_msg(down, j).wait_recv()
            part[i, k, :, at] += relay_y[down, :, at]
            y_msg(4 + down, j).start()

    def pass_x():
        for down, k, t in ((0, 1, 1), (1, 3, 0)):
            x_msg(down).wait_recv()
            acc[k, t] += relay_x[down]
            x_msg(4 + down).start()

    pass_y(0)
    pass_x()
    for j in range(1, n):
        pass_y(j)

    def mine_of(e):
        return own.at[e] if e < 2 else part.at[3 - e, 0]

    def out_y(e, j):
        return lcopy(mine_of(e).at[:, pl.ds(*subs[j])], dw_ref.at[:, cut(e, j)], loc_o.at[e % 2])

    def done_y(pair):
        for j in range(n):
            at = pl.ds(*subs[j])
            for e in pair:
                y_msg((5, 4, 2, 3)[e], j).wait_recv()
                mine_of(e)[:, at] += tail_y[(2, 3, 1, 0)[e], :, at]
                if j:
                    out_y(e, j - 1).wait()
                out_y(e, j).start()
        for e in pair:
            out_y(e, n - 1).wait()

    done_y((3, 2))
    for t in range(2):
        for m in ((2, 5) if t == 0 else (3, 4)):
            x_msg(m).wait_recv()
        rows = pl.ds(t * deep, deep)
        buf[1, rows, 0:quarter] = (acc[0, t] + tail_x[t, 0] + tail_x[t, 1]).astype(BF16)
        lcopy(buf.at[1, rows, pl.ds(0, quarter)], dx_ref.at[rows], loc_dx.at[t]).start()
    x_partner().wait_send()
    for up in range(2):
        for core in range(2):
            x_side(up, core).wait_send()

            @pl.when(near(0) != 0)
            def _(up=up, core=core):
                x_rows(up, core).wait_send()
        x_pass(0, up).wait_send()
        for row in (1, 2):
            @pl.when(used(row, 3 if up else 1))
            def _(row=row, up=up):
                x_pass(row, up).wait_send()

            @pl.when(used(row, 0))
            def _(row=row, up=up):
                x_next(row, up).wait_send()
    for t in range(2):
        rows = pl.ds(t * deep, deep)
        lcopy(buf.at[1, rows, pl.ds(0, quarter)], dx_ref.at[rows], loc_dx.at[t]).wait()
        w_swap(t).wait_send()
    dy_swap().wait_send()
    for m in range(6):
        x_msg(m).wait_send()
    for j in range(n):
        for side in range(2):
            dy_give(side, j).wait_send()
            dy_share(side, j, mine).wait_send()
        for m in range(4):
            y_msg(m, j).wait_send()
    done_y((0, 1))
    for j in range(n):
        for m in (4, 5):
            y_msg(m, j).wait_send()


def finish(dx_in, dw_in, dx_ref, dw_ref, dx_v, dw_v, sem_in, sem_out):
    rows = dw_in.shape[0] // PARTS

    def piece(i):
        if i < PARTS:
            at = pl.ds(i * rows, rows)
            return dw_in.at[at], dw_v.at[at], dw_ref.at[at]
        return dx_in, dx_v, dx_ref

    def load(i):
        return pltpu.make_async_copy(*piece(i)[:2], sem_in.at[i])

    def store(i):
        return pltpu.make_async_copy(*piece(i)[1:], sem_out.at[i])

    for i in range(PARTS + 1):
        load(i).start()
    for i in range(PARTS + 1):
        load(i).wait()
        store(i).start()
    for i in range(PARTS + 1):
        store(i).wait()


def solution(mesh):
    act_spec = P(("pod", "data", "row"), "col")
    wgt_spec = P(("pod", "row"), "col")
    nd, nc, nr = mesh.shape["data"], mesh.shape["col"], mesh.shape["row"]

    def local_step(x_blk, w_blk, dy_blk):
        tokens, feats = x_blk.shape
        cols = dy_blk.shape[1]
        band = feats // nr
        span = pl.cdiv(cols, 128 * nd) * 128
        n = len(pieces(span))
        any_spec = pl.BlockSpec(memory_space=pl.ANY)
        dma = pltpu.SemaphoreType.DMA
        outs = pl.pallas_call(
            functools.partial(kernel, nd, nc),
            out_shape=(
                jax.ShapeDtypeStruct((tokens, feats), BF16),
                jax.ShapeDtypeStruct((band, cols), F32),
                jax.ShapeDtypeStruct((tokens, cols), BF16),
                jax.ShapeDtypeStruct(w_blk.shape, BF16),
                jax.ShapeDtypeStruct((2, 2 * tokens, span), BF16),
            ),
            in_specs=[any_spec] * 3,
            out_specs=(any_spec,) * 5,
            scratch_shapes=[
                pltpu.VMEM((tokens, feats), BF16),
                pltpu.VMEM((feats, tokens), BF16),
                pltpu.VMEM((3, 4, band, 2 * tokens), BF16),
                pltpu.VMEM((2, 4, band, span), F32),
                pltpu.VMEM((2, band, span), F32),
                pltpu.VMEM((2, band, span), F32),
                pltpu.VMEM((4, band, span), F32),
                pltpu.VMEM((4, 2, tokens // 2, feats), F32),
                pltpu.VMEM((2, tokens // 2, feats), F32),
                pltpu.VMEM((2, 2, tokens // 2, feats), F32),
                pltpu.VMEM((2, 2 * tokens, 2 * DEPTH), BF16),
                dma(()), dma((2, 2)), dma((2, 2)), dma((3, 4, 2)), dma((2, 2)), dma((2, 2)), dma((3, 2)), dma(()),
                dma(()), dma(()), dma((2,)), dma((2,)),
                dma((2, n)), dma((2, n)), dma((2, n)), dma((2, n)), dma((2, 2)), dma((2,)),
                dma((6, n)), dma((6, n)), dma((6,)), dma((6,)), dma((2,)), dma((2, 3)), dma((2,)),
            ],
            compiler_params=pltpu.CompilerParams(
                collective_id=0, has_side_effects=True, vmem_limit_bytes=67043328),
        )(x_blk, w_blk, dy_blk)
        return pl.pallas_call(
            finish,
            out_shape=(
                jax.ShapeDtypeStruct((tokens, feats), BF16),
                jax.ShapeDtypeStruct((band, cols), F32),
            ),
            in_specs=[any_spec] * 2,
            out_specs=(any_spec,) * 2,
            scratch_shapes=[
                pltpu.VMEM((tokens, feats), BF16),
                pltpu.VMEM((band, cols), F32),
                dma((PARTS + 1,)), dma((PARTS + 1,)),
            ],
            compiler_params=pltpu.CompilerParams(vmem_limit_bytes=67043328),
        )(outs[0], outs[1])

    return jax.shard_map(local_step, mesh=mesh, in_specs=(act_spec, wgt_spec, act_spec),
                         out_specs=(act_spec, act_spec), check_vma=False)
```
